32 devices in a mesh: rep: 2 (over x), dp: 16 (over y, z, core).
Axes of the slice: x: 2, y: 2, z: 4, core: 2. Of those that a mesh axis runs over, the one named last changes fastest.
Arguments:
- x: bfloat16 [32, 2048, 1024], P(('rep', 'dp')), parts along dimension 0
- dy: bfloat16 [32, 2048, 1024], P(('rep', 'dp')), parts along dimension 0
- w_gate: bfloat16 [2, 1024, 3328], P(None, 'dp')
- w_up: bfloat16 [2, 1024, 3328], P(None, 'dp')
- w_down: bfloat16 [2, 3328, 1024], P(None, 'dp')
- m_w_gate: float32 [2, 1024, 3328], P(None, 'dp')
- m_w_up: float32 [2, 1024, 3328], P(None, 'dp')
- m_w_down: float32 [2, 3328, 1024], P(None, 'dp')
- v_w_gate: float32 [2, 1024, 3328], P(None, 'dp')
- v_w_up: float32 [2, 1024, 3328], P(None, 'dp')
- v_w_down: float32 [2, 3328, 1024], P(None, 'dp')
Outputs:
- output 1: bfloat16 [4, 1024, 3328], P('rep', 'dp'), parts along dimension 0
- output 2: bfloat16 [4, 1024, 3328], P('rep', 'dp'), parts along dimension 0
- output 3: bfloat16 [4, 3328, 1024], P('rep', 'dp'), parts along dimension 0
- output 4: float32 [4, 1024, 3328], P('rep', 'dp'), parts along dimension 0
- output 5: float32 [4, 1024, 3328], P('rep', 'dp'), parts along dimension 0
- output 6: float32 [4, 3328, 1024], P('rep', 'dp'), parts along dimension 0
- output 7: float32 [4, 1024, 3328], P('rep', 'dp'), parts along dimension 0
- output 8: float32 [4, 1024, 3328], P('rep', 'dp'), parts along dimension 0
- output 9: float32 [4, 3328, 1024], P('rep', 'dp'), parts along dimension 0
There are 2 independent parts. The reference program is written for one: setup_inputs(seed, part) draws one part's arguments, and reference() takes and returns one part's arrays. A program takes and returns all parts, laid end to end along the dimension named above; an argument that names none is the same for every part.
All inputs are finite; a program needn't handle non-finite values.
Results may differ from the reference program's by a relative error of at most 0.022.
Values are sent between devices in bfloat16 or wider.
A program may use at most 2 GiB of HBM per device.

```python
import jax
import jax.numpy as jnp
from jax import lax

SEQUENCES = 16
TOKENS = 2048
D = 1024
FF = 3328
LAYERS = 2
NAMES = ("w_gate", "w_up", "w_down")
SHAPES = {"w_gate": (LAYERS, D, FF), "w_up": (LAYERS, D, FF), "w_down": (LAYERS, FF, D)}


def bump(key, n, height):
    away = (jnp.arange(n, dtype=jnp.int32) - jax.random.randint(key, (), 0, n, jnp.int32)) % n
    return jnp.where(away < n // 8, height, 1.0)


def together(key, own, strength):
    shared = jax.random.normal(key, own.shape[1:], jnp.float32)
    return (own + strength * shared) * lax.rsqrt(1 + strength * strength)


def setup_inputs(seed: int = 0, part: int = 0) -> dict:
    kx, kdy, ka, kb, kz, kf, kh, kl, *keys = jax.random.split(jax.random.key(seed), 8 + 3 * len(NAMES))
    kx, kdy, ka, kb = (jax.random.fold_in(k, part) for k in (kx, kdy, ka, kb))
    kw, km, kv = (keys[i::3] for i in range(3))
    shape = (SEQUENCES, TOKENS, D)
    much_x, much_dy = jax.random.uniform(kz, (2,), jnp.float32, 0.0, 1.0)
    loud = 2.0 ** jax.random.uniform(jax.random.fold_in(kz, 1), (), jnp.float32, -1.0, 2.0)
    layers = 2.0 ** jax.random.uniform(kl, (LAYERS, 1, 1), jnp.float32, -1.0, 1.0)
    x = together(ka, jax.random.normal(kx, shape, jnp.float32), much_x) * bump(kf, D, 4.0)
    dy = together(kb, jax.random.normal(kdy, shape, jnp.float32), much_dy)
    drawn = {"x": x.astype(jnp.bfloat16), "dy": (loud * dy * (SEQUENCES * TOKENS) ** -0.5).astype(jnp.bfloat16)}
    for key, name in zip(kw, NAMES, strict=True):
        w = jax.random.normal(key, SHAPES[name], jnp.float32) * SHAPES[name][1] ** -0.5
        drawn[name] = (w * {"w_gate": 1.0, "w_up": bump(kh, FF, 4.0), "w_down": layers}[name]).astype(jnp.bfloat16)
    for key, name in zip(km, NAMES, strict=True):
        drawn[f"m_{name}"] = 0.1 * jax.random.normal(key, SHAPES[name], jnp.float32)
    for key, name in zip(kv, NAMES, strict=True):
        drawn[f"v_{name}"] = jax.random.uniform(key, SHAPES[name], jnp.float32, 0.005, 0.015)
    return drawn


def matmul(a, w):
    return jnp.dot(a, w, preferred_element_type=jnp.float32).astype(jnp.bfloat16)


def normed(h):
    wide = h.astype(jnp.float32)
    scale = lax.rsqrt(jnp.mean(wide**2, -1, keepdims=True) + 1e-6)
    return (wide * scale).astype(jnp.bfloat16)


def layer(h, w):
    a = normed(h)
    gate = jnp.dot(a, w["w_gate"], preferred_element_type=jnp.float32)
    up = jnp.dot(a, w["w_up"], preferred_element_type=jnp.float32)
    return h + matmul((jax.nn.silu(gate) * up).astype(jnp.bfloat16), w["w_down"])


def adamw(w, m, v, g):
    m = 0.9 * m + 0.1 * g
    v = 0.95 * v + 0.05 * g * g
    step = m * lax.rsqrt(v + 1e-8) + 0.1 * w
    return (w - 0.02 * step).astype(jnp.bfloat16), m, v


def clipped(gradients, sum_of_squares, count):
    factor = jnp.minimum(1.0, 0.5 * lax.rsqrt(sum_of_squares / count + 1e-30))
    return [g * factor for g in gradients]


def stack(weights, h):
    return lax.scan(lambda h, w: (layer(h, w), None), h, weights)[0]


def reference(x, dy, w_gate, w_up, w_down, m_w_gate, m_w_up, m_w_down, v_w_gate, v_w_up, v_w_down):
    weights = dict(zip(NAMES, (w_gate, w_up, w_down), strict=True))

    def take(so_far, sequence):
        h, by_y = sequence
        _, back = jax.vjp(lambda w: stack(w, h), weights)
        return jax.tree.map(lambda total, term: total + term.astype(jnp.float32), so_far, back(by_y)[0]), None

    none_yet = {name: jnp.zeros(w.shape, jnp.float32) for name, w in weights.items()}
    by_weights, _ = lax.scan(take, none_yet, (x, dy))
    gradients = [by_weights[name].astype(jnp.bfloat16).astype(jnp.float32) for name in NAMES]
    gradients = clipped(gradients, sum(jnp.sum(g * g) for g in gradients), sum(g.size for g in gradients))
    new = [
        adamw(w.astype(jnp.float32), m, v, g)
        for w, m, v, g in zip((w_gate, w_up, w_down), (m_w_gate, m_w_up, m_w_down), (v_w_gate, v_w_up, v_w_down), gradients, strict=True)
    ]
    return tuple(one[which] for which in range(3) for one in new)
```

```python
import functools

import jax
import jax.numpy as jnp
from jax import lax
from jax.experimental import pallas as pl
from jax.experimental.pallas import tpu as pltpu
from jax.sharding import PartitionSpec as P

BF16, F32 = jnp.bfloat16, jnp.float32
MIB = 1 << 20
CHIPS = 8
ANY = pl.BlockSpec(memory_space=pl.ANY)


def order(q):
    return q + lax.div(q, 4) * (11 - 2 * q)


class Here:
    def __init__(self):
        me = lax.axis_index("dp")
        self.me, self.c = me, lax.rem(me, 2)
        self.p = order(lax.div(me, 2))
        self.sibling = {"dp": 2 * lax.div(me, 2) + 1 - self.c}
        self.hops = (4 - self.c, 3 + self.c)
        self.next = tuple({"dp": 2 * self.chip(o) + self.c} for o in (1, CHIPS - 1))

    def chip(self, offset):
        return order(lax.rem(self.p + offset, CHIPS))


def remote(src, dst, send, recv, to):
    return pltpu.make_async_remote_copy(src, dst, send, recv, device_id=to, device_id_type=pl.DeviceIdType.MESH)


def greet(here):
    barrier = pltpu.get_barrier_semaphore()
    for to in (here.sibling, *here.next):
        pl.semaphore_signal(barrier, inc=1, device_id=to, device_id_type=pl.DeviceIdType.MESH)
    pl.semaphore_wait(barrier, 3)


class Gather:
    def __init__(self, shapes, cuts):
        self.shapes, self.cuts = shapes, cuts
        self.units = [(m, i, shape[0], shape[1] // cuts) for m, shape in enumerate(shapes) for i in range(cuts)]
        n = len(self.units)
        self.rounds = 5 * n
        dma = pltpu.SemaphoreType.DMA
        self.scratch = [dma((n, 2, 4)), dma((n, 2, 4)), dma((n, CHIPS)), dma((n, CHIPS)), dma((len(shapes),))]
        self.scratch += [pltpu.VMEM(shape, BF16) for shape in shapes]
        self.out_shapes = [jax.ShapeDtypeStruct((2 * CHIPS * r, c), BF16) for r, c in shapes]

    def bind(self, ins, outs, scratch):
        self.ins, self.outs = ins, outs
        self.send, self.recv, self.dsend, self.drecv, self.local = scratch[:5]
        self.held = scratch[5:]

    def block(self, here, u, offset, core):
        m, i, rows, cols = self.units[u]
        start = pl.multiple_of((2 * here.chip(offset) + core) * rows, 16)
        return self.outs[m].at[pl.ds(start, rows), pl.ds(i * cols, cols)]

    def own(self, u):
        m, i, rows, cols = self.units[u]
        return self.ins[m].at[:, pl.ds(i * cols, cols)]

    def start(self, here):
        greet(here)
        for m in range(len(self.shapes)):
            pltpu.make_async_copy(self.ins[m], self.held[m], self.local.at[m]).start()

    def unit(self, here, u, h):
        @pl.when(h == 0)
        def _():
            mine, dst = self.own(u), self.block(here, u, 0, here.c)
            for d in range(2):
                remote(mine, dst, self.send.at[u, d, 0], self.recv.at[u, d, 0], here.next[d]).start()
            remote(mine, dst, self.dsend.at[u, 0], self.drecv.at[u, 0], here.sibling).start()

        for d in range(2):
            offset = lax.rem(CHIPS - h, CHIPS) if d == 0 else h
            blk = self.block(here, u, offset, here.c)

            @pl.when((h >= 1) & (h <= here.hops[d]))
            def _():
                remote(blk, blk, self.send.at[u, d, h - 1], self.recv.at[u, d, h - 1], here.next[d]).wait_recv()

            @pl.when((h >= 1) & (h < here.hops[d]))
            def _():
                remote(blk, blk, self.send.at[u, d, h], self.recv.at[u, d, h], here.next[d]).start()

            @pl.when((h >= 1) & (h <= here.hops[d]))
            def _():
                remote(blk, blk, self.dsend.at[u, offset], self.drecv.at[u, offset], here.sibling).start()

    def round(self, here, r):
        n = len(self.units)
        for u in range(n):
            pl.when(lax.rem(r, n) == u)(functools.partial(self.unit, here, u, lax.div(r, n)))

    def finish(self, here):
        for m, (rows, cols) in enumerate(self.shapes):
            mine = self.outs[m].at[pl.ds(pl.multiple_of(here.me * rows, 16), rows), :]
            pltpu.make_async_copy(self.ins[m], self.held[m], self.local.at[m]).wait()
            pltpu.make_async_copy(self.held[m], mine, self.local.at[m]).start()
        for u in range(len(self.units)):

            @pl.loop(0, CHIPS)
            def _(o):
                blk = self.block(here, u, o, here.c)
                remote(blk, blk, self.dsend.at[u, o], self.drecv.at[u, o], here.sibling).wait()

            for d in range(2):

                @pl.loop(0, here.hops[d])
                def _(h):
                    blk = self.block(here, u, 0, here.c)
                    remote(blk, blk, self.send.at[u, d, h], self.recv.at[u, d, h], here.next[d]).wait_send()

        for m, (rows, cols) in enumerate(self.shapes):
            mine = self.outs[m].at[pl.ds(pl.multiple_of(here.me * rows, 16), rows), :]
            pltpu.make_async_copy(self.held[m], mine, self.local.at[m]).wait()


class Scatter:
    def __init__(self, shapes, cuts):
        self.shapes, self.cuts = shapes, cuts
        self.units = [(m, i, shape[0], shape[1] // cuts) for m, shape in enumerate(shapes) for i in range(cuts)]
        n = len(self.units)
        self.rounds = 5 * n
        dma = pltpu.SemaphoreType.DMA
        self.scratch = [dma((n, 2, 4)), dma((n, 2, 4)), dma((n, CHIPS)), dma((n, CHIPS)), dma((n, CHIPS))]
        for _, _, rows, cols in self.units:
            self.scratch += [pltpu.VMEM((CHIPS, rows, cols), BF16)] * 2 + [pltpu.VMEM((2, 4, rows, cols), BF16)]
        self.scratch += [pltpu.VMEM(shape, BF16) for shape in shapes] + [dma((len(shapes),))]
        self.out_shapes = [jax.ShapeDtypeStruct(shape, BF16) for shape in shapes]

    def bind(self, ins, outs, scratch):
        self.ins, self.outs = ins, outs
        self.send, self.recv, self.dsend, self.drecv, self.local = scratch[:5]
        n = len(self.units)
        self.mine, self.theirs, self.came = (scratch[5 + j : 5 + 3 * n : 3] for j in range(3))
        self.total = scratch[5 + 3 * n : -1]
        self.put = scratch[-1]

    def term(self, here, u, offset, core):
        m, i, rows, cols = self.units[u]
        start = pl.multiple_of((2 * here.chip(offset) + core) * rows, 16)
        return self.ins[m].at[pl.ds(start, rows), pl.ds(i * cols, cols)]

    def fetch(self, here, u, o):
        return pltpu.make_async_copy(self.term(here, u, o, here.c), self.mine[u].at[o], self.local.at[u, o])

    def give(self, here, u, o):
        term = self.term(here, u, o, 1 - here.c)
        return remote(term, self.theirs[u].at[o], self.dsend.at[u, o], self.drecv.at[u, o], here.sibling)

    def start(self, here):
        greet(here)

        @pl.loop(0, CHIPS)
        def _(j):
            odd, half = lax.rem(j, 2), lax.div(j, 2)
            o = lax.rem((1 - odd) * (4 - half) + odd * (5 + half), CHIPS)
            for u in range(len(self.units)):
                self.give(here, u, o).start()
                self.fetch(here, u, o).start()

    def unit(self, here, u, k):
        m, i, rows, cols = self.units[u]
        mine, theirs, came = self.mine[u], self.theirs[u], self.came[u]
        for d in range(2):
            far = here.hops[d] - k
            o = far if d == 0 else CHIPS - far

            @pl.when(k < here.hops[d])
            def _():
                self.fetch(here, u, o).wait()
                self.give(here, u, o).wait_recv()

            @pl.when((k < here.hops[d]) & (k == 0))
            def _():
                mine[o] = (mine[o].astype(F32) + theirs[o].astype(F32)).astype(BF16)

            @pl.when((k < here.hops[d]) & (k > 0))
            def _():
                remote(mine.at[o], came.at[d, k - 1], self.send.at[u, d, k - 1], self.recv.at[u, d, k - 1], here.next[d]).wait_recv()
                mine[o] = (mine[o].astype(F32) + theirs[o].astype(F32) + came[d, k - 1].astype(F32)).astype(BF16)

            @pl.when(k < here.hops[d])
            def _():
                remote(mine.at[o], came.at[d, k], self.send.at[u, d, k], self.recv.at[u, d, k], here.next[d]).start()

        @pl.when(k == 4)
        def _():
            self.fetch(here, u, 0).wait()
            self.give(here, u, 0).wait_recv()
            total = mine[0].astype(F32) + theirs[0].astype(F32)
            for d in range(2):
                last = here.hops[d] - 1
                remote(mine.at[0], came.at[d, last], self.send.at[u, d, last], self.recv.at[u, d, last], here.next[d]).wait_recv()
                total += came[d, last].astype(F32)
            self.total[m][:, pl.ds(i * cols, cols)] = total.astype(BF16)

    def round(self, here, r):
        n = len(self.units)
        for u in range(n):
            pl.when(lax.rem(r, n) == u)(functools.partial(self.unit, here, u, lax.div(r, n)))

    def finish(self, here):
        for m in range(len(self.shapes)):
            pltpu.make_async_copy(self.total[m], self.outs[m], self.put.at[m]).start()
        for u in range(len(self.units)):

            @pl.loop(0, CHIPS)
            def _(o):
                self.give(here, u, o).wait_send()

            for d in range(2):

                @pl.loop(0, here.hops[d])
                def _(k):
                    remote(
                        self.mine[u].at[0], self.came[u].at[d, k], self.send.at[u, d, k], self.recv.at[u, d, k], here.next[d]
                    ).wait_send()

        for m in range(len(self.shapes)):
            pltpu.make_async_copy(self.total[m], self.outs[m], self.put.at[m]).wait()


def hosted(name, body, steps, marks, in_specs, out_specs, out_shape, args, carried=None, carried_args=(), number=None, scratch=(), limit=60):
    n_in, n_out, n_scratch = len(in_specs), len(out_specs), len(scratch)
    n_cin = len(carried_args)
    c_out = carried.out_shapes if carried else []

    def kernel(*refs):
        ins, refs = refs[:n_in], refs[n_in:]
        cin, refs = refs[:n_cin], refs[n_cin:]
        outs, refs = refs[:n_out], refs[n_out:]
        couts, refs = refs[: len(c_out)], refs[len(c_out) :]
        own, refs = refs[:n_scratch], refs[n_scratch:]
        step = pl.program_id(0)
        if carried is None:
            body(ins, outs, own, lambda j: None)
            return
        here = Here()
        carried.bind(cin, couts, refs)
        pl.when(step == 0)(functools.partial(carried.start, here))
        total = steps * marks

        def mark(j):
            at = step * marks + j

            @pl.loop(lax.div(at * carried.rounds, total), lax.div((at + 1) * carried.rounds, total))
            def _(r):
                carried.round(here, r)

        if body is None:
            mark(0)
        else:
            body(ins, outs, own, mark)
        pl.when(step == steps - 1)(functools.partial(carried.finish, here))

    params = dict(vmem_limit_bytes=limit * MIB, dimension_semantics=("arbitrary",))
    if carried is not None:
        params |= dict(collective_id=number, has_side_effects=True)
    out = pl.pallas_call(
        kernel,
        grid=(steps,),
        in_specs=[*in_specs, *[ANY] * n_cin],
        out_specs=[*out_specs, *[ANY] * len(c_out)],
        out_shape=[*out_shape, *c_out],
        scratch_shapes=[*scratch, *(carried.scratch if carried else [])],
        compiler_params=pltpu.CompilerParams(**params),
        name=name,
    )(*args, *carried_args)
    return out[:n_out], out[n_out:]


def whole(shape):
    return pl.BlockSpec(shape, lambda i: (0, 0), pipeline_mode=pl.Buffered(1))


def dot(a, b, over):
    return lax.dot_general(a, b, ((over[:1], over[1:]), ((), ())), preferred_element_type=F32)


def scaled(h):
    wide = h.astype(F32)
    return (wide * lax.rsqrt(jnp.mean(wide * wide, -1, keepdims=True) + 1e-6)).astype(BF16)


def up_kernel(a, wg, wu, **carry):
    t, d = a.shape
    ff = wg.shape[1]
    n, part = 256, 512

    def body(ins, outs, own, mark):
        a, wg, wu = ins
        act, s, v = outs
        for j in range(t // part):
            rows = pl.ds(j * part, part)
            g = dot(a[rows, :], wg[...], (1, 0))
            u = dot(a[rows, :], wu[...], (1, 0))
            sig = jax.nn.sigmoid(g)
            sl = g * sig
            act[rows, :] = (sl * u).astype(BF16)
            s[rows, :] = sl
            v[rows, :] = u * (sig * (1.0 + g * (1.0 - sig)))
            mark(j)

    col = lambda rows: pl.BlockSpec((rows, n), lambda i: (0, i))
    return hosted(
        "up", body, ff // n, t // part, [whole((t, d)), col(d), col(d)], [col(t)] * 3,
        [jax.ShapeDtypeStruct((t, ff), x) for x in (BF16, F32, F32)], (a, wg, wu), **carry,
    )


def down_kernel(act, wd, h, **carry):
    t, ff = act.shape
    d = wd.shape[1]
    m, n = 512, 256

    def body(ins, outs, own, mark):
        act, wd, h = ins
        new, a = outs
        for j in range(d // n):
            cols = pl.ds(j * n, n)
            new[:, cols] = h[:, cols] + dot(act[...], wd[:, cols], (1, 0)).astype(BF16)
            mark(j)
        a[...] = scaled(new[...])

    row = lambda cols: pl.BlockSpec((m, cols), lambda i: (i, 0))
    return hosted(
        "down", body, t // m, d // n, [row(ff), whole((ff, d)), row(d)], [row(d)] * 2,
        [jax.ShapeDtypeStruct((t, d), BF16)] * 2, (act, wd, h), **carry,
    )


def back_kernel(at, dh, wd, act, s, v, keep, **carry):
    d, t = at.shape
    ff = act.shape[1]
    n, part = 256, 512

    def body(ins, outs, own, mark):
        at, dh, wd, act, s, v = ins
        by_g, by_u, by_wd, by_wg, by_wu = outs if keep else (*own, *outs)
        for j in range(t // part):
            rows = pl.ds(j * part, part)
            by_act = dot(dh[rows, :], wd[...], (1, 1)).astype(BF16).astype(F32)
            by_g[rows, :] = (by_act * v[rows, :]).astype(BF16)
            by_u[rows, :] = (by_act * s[rows, :]).astype(BF16)
        mark(0)
        by_wd[...] = dot(act[...], dh[...], (0, 0)).astype(BF16)
        mark(1)
        by_wg[...] = dot(at[...], by_g[...], (1, 0)).astype(BF16)
        mark(2)
        by_wu[...] = dot(at[...], by_u[...], (1, 0)).astype(BF16)
        mark(3)

    col = lambda rows: pl.BlockSpec((rows, n), lambda i: (0, i))
    row = pl.BlockSpec((n, d), lambda i: (i, 0))
    shape = lambda *s: jax.ShapeDtypeStruct(s, BF16)
    return hosted(
        "back", body, ff // n, 4, [whole((d, t)), whole((t, d)), row, col(t), col(t), col(t)],
        [col(t)] * (2 * keep) + [row, col(d), col(d)],
        [shape(t, ff)] * (2 * keep) + [shape(ff, d), shape(d, ff), shape(d, ff)],
        (at, dh, wd, act, s, v), scratch=() if keep else [pltpu.VMEM((t, n), BF16)] * 2, **carry,
    )


def through_kernel(by_g, by_u, wg, wu, h, dh, **carry):
    t, ff = by_g.shape
    d = wg.shape[0]
    m, n = 256, 256

    def body(ins, outs, own, mark):
        by_g, by_u, wg, wu, h, dh = ins
        (new,) = outs
        (by_a,) = own
        for j in range(d // n):
            cols = pl.ds(j * n, n)
            one = dot(by_g[...], wg[cols, :], (1, 1)).astype(BF16)
            two = dot(by_u[...], wu[cols, :], (1, 1)).astype(BF16)
            by_a[:, cols] = (one + two).astype(F32)
            mark(j)
        wide, by = h[...].astype(F32), by_a[...]
        scale = lax.rsqrt(jnp.mean(wide * wide, -1, keepdims=True) + 1e-6)
        inner = jnp.mean(wide * by, -1, keepdims=True)
        new[...] = dh[...] + (by * scale - wide * (scale * scale * scale * inner)).astype(BF16)

    row = lambda cols: pl.BlockSpec((m, cols), lambda i: (i, 0))
    return hosted(
        "through", body, t // m, d // n, [row(ff), row(ff), whole((d, ff)), whole((d, ff)), row(d), row(d)], [row(d)],
        [jax.ShapeDtypeStruct((t, d), BF16)], (by_g, by_u, wg, wu, h, dh), scratch=[pltpu.VMEM((m, d), F32)], **carry,
    )


def alone(name, **carry):
    return hosted(name, None, 1, 1, [], [], [], (), **carry)[1]


def adamw(w, m, v, g):
    m = 0.9 * m + 0.1 * g
    v = 0.95 * v + 0.05 * g * g
    step = m * lax.rsqrt(v + 1e-8) + 0.1 * w
    return (w - 0.02 * step).astype(BF16), m, v


def clipped(gradients, sum_of_squares, count):
    factor = jnp.minimum(1.0, 0.5 * lax.rsqrt(sum_of_squares / count + 1e-30))
    return [g * factor for g in gradients]


def solution(mesh):
    def step(x, dy, *arrays):
        weights, m, v = (arrays[i : i + 3] for i in (0, 3, 6))
        (g0, g1), (u0, u1), (d0, d1) = ((w[0], w[1]) for w in weights)
        wide, deep = g0.shape, d0.shape
        x, dy = x[0], dy[0]

        a0 = scaled(x)
        wg0, wu0 = alone("gather", carried=Gather([wide, wide], 2), carried_args=(g0, u0), number=1)
        (act0, s0, v0), (wd0,) = up_kernel(a0, wg0, wu0, carried=Gather([deep], 2), carried_args=(d0,), number=2)
        (h1, a1), (wg1, wu1) = down_kernel(act0, wd0, x, carried=Gather([wide, wide], 2), carried_args=(g1, u1), number=3)
        (act1, s1, v1), (wd1,) = up_kernel(a1, wg1, wu1, carried=Gather([deep], 2), carried_args=(d1,), number=4)

        (by_g, by_u, by_d1, by_g1, by_u1), _ = back_kernel(a1.T, dy, wd1, act1, s1, v1, True)
        (dh,), (sd1,) = through_kernel(by_g, by_u, wg1, wu1, h1, dy, carried=Scatter([deep], 2), carried_args=(by_d1,), number=5)
        (by_d0, by_g0, by_u0), (sg1, su1) = back_kernel(
            a0.T, dh, wd0, act0, s0, v0, False, carried=Scatter([wide, wide], 2), carried_args=(by_g1, by_u1), number=6
        )
        sd0, sg0, su0 = alone("scatter", carried=Scatter([deep, wide, wide], 2), carried_args=(by_d0, by_g0, by_u0), number=7)

        mine = ((sg0, sg1), (su0, su1), (sd0, sd1))
        gradients = [jnp.stack(pair).astype(F32) for pair in mine]
        squares = lax.psum(sum(jnp.sum(g * g) for g in gradients), "dp")
        gradients = clipped(gradients, squares, lax.psum(1, "dp") * sum(g.size for g in gradients))
        new = [adamw(w.astype(F32), m, v, g) for w, m, v, g in zip(weights, m, v, gradients, strict=True)]
        return tuple(one[which] for which in range(3) for one in new)

    states, cut = P(("rep", "dp"), None, None), P(None, "dp", None)
    return jax.shard_map(
        step,
        mesh=mesh,
        in_specs=(states, states) + (cut,) * 9,
        out_specs=(P("rep", "dp", None),) * 9,
        check_vma=False,
    )
```

```python
import functools

import jax
import jax.numpy as jnp
from jax import lax
from jax.experimental import pallas as pl
from jax.experimental.pallas import tpu as pltpu
from jax.sharding import PartitionSpec as P

BF16, F32 = jnp.bfloat16, jnp.float32
MIB = 1 << 20
CHIPS = 8
ANY = pl.BlockSpec(memory_space=pl.ANY)


def order(q):
    return q + lax.div(q, 4) * (11 - 2 * q)


class Here:
    def __init__(self):
        me = lax.axis_index("dp")
        self.me, self.c = me, lax.rem(me, 2)
        self.p = order(lax.div(me, 2))
        self.sibling = {"dp": 2 * lax.div(me, 2) + 1 - self.c}
        self.hops = (4 - self.c, 3 + self.c)
        self.rep = lax.axis_index("rep")
        self.twin = {"rep": 1 - self.rep}
        self.next = tuple({"dp": 2 * self.chip(o) + self.c} for o in (1, CHIPS - 1))

    def chip(self, offset):
        return order(lax.rem(self.p + offset, CHIPS))


def remote(src, dst, send, recv, to):
    return pltpu.make_async_remote_copy(src, dst, send, recv, device_id=to, device_id_type=pl.DeviceIdType.MESH)


def greet(*others):
    barrier = pltpu.get_barrier_semaphore()
    for to in others:
        pl.semaphore_signal(barrier, inc=1, device_id=to, device_id_type=pl.DeviceIdType.MESH)
    pl.semaphore_wait(barrier, len(others))


class Gather:
    def __init__(self, shapes, units, number):
        self.shapes, self.number = shapes, number
        self.units = [(m, at, side, ring) for m, at, side, ring in units]
        n = len(self.units)
        self.rounds = 6 * n
        dma = pltpu.SemaphoreType.DMA
        self.scratch = [dma((n, 2, 4)), dma((n, 2, 4)), *[dma((n, CHIPS))] * 6, dma((len(shapes),))]
        self.scratch += [pltpu.VMEM(shape, BF16) for shape in shapes]
        self.out_shapes = [jax.ShapeDtypeStruct((2 * CHIPS * r, c), BF16) for r, c in shapes]

    def bind(self, ins, outs, scratch):
        self.ins, self.outs = [ref.at[self.number] for ref in ins], outs
        self.send, self.recv, self.dsend, self.drecv, self.xsend, self.xrecv, self.tsend, self.trecv, self.local = scratch[:9]
        self.held = scratch[9:]

    def columns(self, here, u, kind):
        m, at, side, ring = self.units[u]
        if kind == "all":
            return pl.ds(at, side + ring)
        if kind == "ring":
            return pl.ds(pl.multiple_of(at + here.rep * side, 128), ring)
        rep = here.rep if kind == "gives" else 1 - here.rep
        return pl.ds(pl.multiple_of(at + rep * ring, 128), side)

    def block(self, here, u, offset, kind):
        m = self.units[u][0]
        rows = self.shapes[m][0]
        start = pl.multiple_of((2 * here.chip(offset) + here.c) * rows, 16)
        return self.outs[m].at[pl.ds(start, rows), self.columns(here, u, kind)]

    def own(self, here, u, kind):
        return self.ins[self.units[u][0]].at[:, self.columns(here, u, kind)]

    def start(self, here):
        greet(here.sibling, here.twin, *here.next)
        for m in range(len(self.shapes)):
            pltpu.make_async_copy(self.ins[m], self.held[m], self.local.at[m]).start()

    def unit(self, here, u, h):
        @pl.when(h == 0)
        def _():
            mine, dst = self.own(here, u, "ring"), self.block(here, u, 0, "ring")
            for d in range(2):
                remote(mine, dst, self.send.at[u, d, 0], self.recv.at[u, d, 0], here.next[d]).start()
            mine, dst = self.own(here, u, "all"), self.block(here, u, 0, "all")
            remote(mine, dst, self.dsend.at[u, 0], self.drecv.at[u, 0], here.sibling).start()

        for d in range(2):
            offset = lax.rem(CHIPS - h, CHIPS) if d == 0 else lax.rem(h, CHIPS)
            blk = self.block(here, u, offset, "ring")

            @pl.when((h >= 1) & (h <= here.hops[d]))
            def _():
                remote(blk, blk, self.send.at[u, d, h - 1], self.recv.at[u, d, h - 1], here.next[d]).wait_recv()

            @pl.when((h >= 1) & (h < here.hops[d]))
            def _():
                remote(blk, blk, self.send.at[u, d, h], self.recv.at[u, d, h], here.next[d]).start()

            @pl.when((h >= 1) & (h <= here.hops[d]))
            def _():
                part = self.block(here, u, offset, "gives")
                remote(part, part, self.xsend.at[u, offset], self.xrecv.at[u, offset], here.twin).start()
                remote(blk, blk, self.dsend.at[u, offset], self.drecv.at[u, offset], here.sibling).start()

        for d in range(2):
            before = lax.rem(CHIPS + 1 - h, CHIPS) if d == 0 else lax.rem(CHIPS + h - 1, CHIPS)

            @pl.when((h >= 2) & (h - 1 <= here.hops[d]))
            def _():
                part = self.block(here, u, before, "gets")
                remote(part, part, self.xsend.at[u, before], self.xrecv.at[u, before], here.twin).wait_recv()
                remote(part, part, self.tsend.at[u, before], self.trecv.at[u, before], here.sibling).start()

    def round(self, here, r):
        n = len(self.units)
        for u in range(n):
            pl.when(lax.rem(r, n) == u)(functools.partial(self.unit, here, u, lax.div(r, n)))

    def rows(self, here, m):
        rows = self.shapes[m][0]
        return self.outs[m].at[pl.ds(pl.multiple_of(here.me * rows, 16), rows), :]

    def finish(self, here):
        for m in range(len(self.shapes)):
            pltpu.make_async_copy(self.ins[m], self.held[m], self.local.at[m]).wait()
            pltpu.make_async_copy(self.held[m], self.rows(here, m), self.local.at[m]).start()
        for u in range(len(self.units)):
            blk = self.block(here, u, 0, "all")
            remote(blk, blk, self.dsend.at[u, 0], self.drecv.at[u, 0], here.sibling).wait()

            @pl.loop(1, CHIPS)
            def _(o):
                blk = self.block(here, u, o, "ring")
                remote(blk, blk, self.dsend.at[u, o], self.drecv.at[u, o], here.sibling).wait()
                blk = self.block(here, u, o, "gives")
                remote(blk, blk, self.xsend.at[u, o], self.xrecv.at[u, o], here.twin).wait_send()
                blk = self.block(here, u, o, "gets")
                remote(blk, blk, self.tsend.at[u, o], self.trecv.at[u, o], here.sibling).wait()

            for d in range(2):

                @pl.loop(0, here.hops[d])
                def _(h):
                    blk = self.block(here, u, 0, "ring")
                    remote(blk, blk, self.send.at[u, d, h], self.recv.at[u, d, h], here.next[d]).wait_send()

        for m in range(len(self.shapes)):
            pltpu.make_async_copy(self.held[m], self.rows(here, m), self.local.at[m]).wait()


class Scatter:
    def __init__(self, shapes, cuts, everyone=False):
        self.shapes, self.cuts, self.everyone = shapes, cuts, everyone
        self.units = [(m, i, shape[0], shape[1] // cuts) for m, shape in enumerate(shapes) for i in range(cuts)]
        n = len(self.units)
        self.rounds = 5 * n
        dma = pltpu.SemaphoreType.DMA
        self.scratch = [dma((n, 2, 4)), dma((n, 2, 4)), dma((n, CHIPS)), dma((n, CHIPS)), dma((n, CHIPS))]
        for _, _, rows, cols in self.units:
            self.scratch += [pltpu.VMEM((CHIPS, rows, cols), BF16)] * 2 + [pltpu.VMEM((2, 4, rows, cols), BF16)]
        self.scratch += [pltpu.VMEM(shape, BF16) for shape in shapes] + [dma((len(shapes) + 1,))]
        self.scratch += [pltpu.VMEM((8, 128), F32), pltpu.VMEM((2 * CHIPS, 8, 128), F32), dma((2 * CHIPS,)), dma((2 * CHIPS,))]
        self.out_shapes = [*(jax.ShapeDtypeStruct(shape, BF16) for shape in shapes), jax.ShapeDtypeStruct((8, 128), F32)]

    def bind(self, ins, outs, scratch):
        self.ins, self.outs = ins, outs
        self.send, self.recv, self.dsend, self.drecv, self.local = scratch[:5]
        n = len(self.units)
        self.mine, self.theirs, self.came = (scratch[5 + j : 5 + 3 * n : 3] for j in range(3))
        self.total = scratch[5 + 3 * n : -5]
        self.put, self.squares, self.slots, self.psend, self.precv = scratch[-5:]

    def term(self, here, u, offset, core):
        m, i, rows, cols = self.units[u]
        start = pl.multiple_of((2 * here.chip(offset) + core) * rows, 16)
        return self.ins[m].at[pl.ds(start, rows), pl.ds(i * cols, cols)]

    def fetch(self, here, u, o):
        return pltpu.make_async_copy(self.term(here, u, o, here.c), self.mine[u].at[o], self.local.at[u, o])

    def give(self, here, u, o):
        term = self.term(here, u, o, 1 - here.c)
        return remote(term, self.theirs[u].at[o], self.dsend.at[u, o], self.drecv.at[u, o], here.sibling)

    def peer(self, here, j):
        return {"dp": lax.rem(here.me + j, 2 * CHIPS)}

    def start(self, here):
        if self.everyone:
            greet(*(self.peer(here, j) for j in range(1, 2 * CHIPS)))
            pltpu.make_async_copy(self.ins[-1], self.squares, self.put.at[len(self.shapes)]).start()
        else:
            greet(here.sibling, *here.next)
        for k in range(2):
            for u in range(len(self.units)):
                self.ahead(here, u, k)

    def ahead(self, here, u, k):
        for d in range(2):
            far = here.hops[d] - k
            o = lax.rem(far + CHIPS if d == 0 else CHIPS - far, CHIPS)

            @pl.when(k < here.hops[d])
            def _():
                self.give(here, u, o).start()
                self.fetch(here, u, o).start()

    def unit(self, here, u, k):
        m, i, rows, cols = self.units[u]
        mine, theirs, came = self.mine[u], self.theirs[u], self.came[u]
        self.ahead(here, u, k + 2)

        @pl.when(k == 1)
        def _():
            self.give(here, u, 0).start()
            self.fetch(here, u, 0).start()

        for d in range(2):
            far = here.hops[d] - k
            o = lax.rem(far + CHIPS if d == 0 else CHIPS - far, CHIPS)

            @pl.when(k < here.hops[d])
            def _():
                self.fetch(here, u, o).wait()
                self.give(here, u, o).wait_recv()

            @pl.when((k < here.hops[d]) & (k == 0))
            def _():
                mine[o] = (mine[o].astype(F32) + theirs[o].astype(F32)).astype(BF16)

            @pl.when((k < here.hops[d]) & (k > 0))
            def _():
                remote(mine.at[o], came.at[d, k - 1], self.send.at[u, d, k - 1], self.recv.at[u, d, k - 1], here.next[d]).wait_recv()
                mine[o] = (mine[o].astype(F32) + theirs[o].astype(F32) + came[d, k - 1].astype(F32)).astype(BF16)

            @pl.when(k < here.hops[d])
            def _():
                remote(mine.at[o], came.at[d, k], self.send.at[u, d, k], self.recv.at[u, d, k], here.next[d]).start()

        @pl.when(k == 4)
        def _():
            self.fetch(here, u, 0).wait()
            self.give(here, u, 0).wait_recv()
            total = mine[0].astype(F32) + theirs[0].astype(F32)
            for d in range(2):
                last = here.hops[d] - 1
                remote(mine.at[0], came.at[d, last], self.send.at[u, d, last], self.recv.at[u, d, last], here.next[d]).wait_recv()
                total += came[d, last].astype(F32)
            self.total[m][:, pl.ds(i * cols, cols)] = total.astype(BF16)

    def round(self, here, r):
        n = len(self.units)
        for u in range(n):
            pl.when(lax.rem(r, n) == u)(functools.partial(self.unit, here, u, lax.div(r, n)))

    def finish(self, here):
        n = len(self.shapes)
        for m in range(n):
            pltpu.make_async_copy(self.total[m], self.outs[m], self.put.at[m]).start()
        squares = 0.0
        for m in range(n):
            wide = self.total[m][...].astype(F32)
            squares += jnp.sum(wide * wide)
        squares = jnp.full((8, 128), squares, F32)
        if self.everyone:
            pltpu.make_async_copy(self.ins[-1], self.squares, self.put.at[n]).wait()
            self.slots[here.me] = self.squares[...] + squares

            @pl.loop(1, 2 * CHIPS)
            def _(j):
                slot = self.slots.at[here.me]
                remote(slot, slot, self.psend.at[j], self.precv.at[here.me], self.peer(here, j)).start()

            @pl.loop(1, 2 * CHIPS)
            def _(j):
                other = lax.rem(here.me + j, 2 * CHIPS)
                slot = self.slots.at[other]
                remote(slot, slot, self.psend.at[j], self.precv.at[other], self.peer(here, j)).wait()

            squares = jnp.sum(self.slots[...], axis=0)
        self.squares[...] = squares
        pltpu.make_async_copy(self.squares, self.outs[n], self.put.at[n]).start()
        for u in range(len(self.units)):

            @pl.loop(0, CHIPS)
            def _(o):
                self.give(here, u, o).wait_send()

            for d in range(2):

                @pl.loop(0, here.hops[d])
                def _(k):
                    remote(
                        self.mine[u].at[0], self.came[u].at[d, k], self.send.at[u, d, k], self.recv.at[u, d, k], here.next[d]
                    ).wait_send()

        for m in range(n):
            pltpu.make_async_copy(self.total[m], self.outs[m], self.put.at[m]).wait()
        pltpu.make_async_copy(self.squares, self.outs[n], self.put.at[n]).wait()


def hosted(name, body, steps, marks, in_specs, out_specs, out_shape, args, carried=None, carried_args=(), number=None, scratch=(), limit=60):
    n_in, n_out, n_scratch = len(in_specs), len(out_specs), len(scratch)
    n_cin = len(carried_args)
    c_out = carried.out_shapes if carried else []

    def kernel(*refs):
        ins, refs = refs[:n_in], refs[n_in:]
        cin, refs = refs[:n_cin], refs[n_cin:]
        outs, refs = refs[:n_out], refs[n_out:]
        couts, refs = refs[: len(c_out)], refs[len(c_out) :]
        own, refs = refs[:n_scratch], refs[n_scratch:]
        step = pl.program_id(0)
        if carried is None:
            body(ins, outs, own, lambda j: None)
            return
        here = Here()
        carried.bind(cin, couts, refs)
        pl.when(step == 0)(functools.partial(carried.start, here))
        total = steps * marks

        def mark(j):
            at = step * marks + j

            @pl.loop(lax.div(at * carried.rounds, total), lax.div((at + 1) * carried.rounds, total))
            def _(r):
                carried.round(here, r)

        if body is None:
            mark(0)
        else:
            body(ins, outs, own, mark)
        pl.when(step == steps - 1)(functools.partial(carried.finish, here))

    params = dict(vmem_limit_bytes=limit * MIB, dimension_semantics=("arbitrary",))
    if carried is not None:
        params |= dict(collective_id=number, has_side_effects=True)
    out = pl.pallas_call(
        kernel,
        grid=(steps,),
        in_specs=[*in_specs, *[ANY] * n_cin],
        out_specs=[*out_specs, *[ANY] * len(c_out)],
        out_shape=[*out_shape, *c_out],
        scratch_shapes=[*scratch, *(carried.scratch if carried else [])],
        compiler_params=pltpu.CompilerParams(**params),
        name=name,
    )(*args, *carried_args)
    return out[:n_out], out[n_out:]


def whole(shape):
    return pl.BlockSpec(shape, lambda i: (0, 0), pipeline_mode=pl.Buffered(1))


def dot(a, b, over):
    return lax.dot_general(a, b, ((over[:1], over[1:]), ((), ())), preferred_element_type=F32)


def scaled(h):
    wide = h.astype(F32)
    return (wide * lax.rsqrt(jnp.mean(wide * wide, -1, keepdims=True) + 1e-6)).astype(BF16)


def norm_kernel(x, **carry):
    t, d = x.shape
    m = 512

    def body(ins, outs, own, mark):
        a = scaled(ins[0][...])
        outs[0][...] = a
        outs[1][...] = a.T
        mark(0)

    row = pl.BlockSpec((m, d), lambda i: (i, 0))
    return hosted(
        "norm", body, t // m, 1, [row], [row, pl.BlockSpec((d, m), lambda i: (0, i))],
        [jax.ShapeDtypeStruct((t, d), BF16), jax.ShapeDtypeStruct((d, t), BF16)], (x,), **carry,
    )


def up_kernel(a, wg, wu, dy=None, **carry):
    t, d = a.shape
    ff = wg.shape[1]
    n, part = 256, 512
    last = dy is not None

    def body(ins, outs, own, mark):
        a, wg, wu = ins[:3]
        act, s, v = (*own, *outs[:2]) if last else outs
        for j in range(t // part):
            rows = pl.ds(j * part, part)
            g = dot(a[rows, :], wg[...], (1, 0))
            u = dot(a[rows, :], wu[...], (1, 0))
            sig = jax.nn.sigmoid(g)
            sl = g * sig
            act[rows, :] = (sl * u).astype(BF16)
            s[rows, :] = sl
            v[rows, :] = u * (sig * (1.0 + g * (1.0 - sig)))
        if last:
            outs[2][...] = dot(act[...], ins[3][...], (0, 0)).astype(BF16)
        mark(0)

    col = lambda rows: pl.BlockSpec((rows, n), lambda i: (0, i))
    row = pl.BlockSpec((n, d), lambda i: (i, 0))
    return hosted(
        "up", body, ff // n, 1, [whole((t, d)), col(d), col(d)] + [whole((t, d))] * last,
        [col(t)] * 2 + [row] if last else [col(t)] * 3,
        [jax.ShapeDtypeStruct((t, ff), F32)] * 2 + [jax.ShapeDtypeStruct((ff, d), BF16)]
        if last else [jax.ShapeDtypeStruct((t, ff), x) for x in (BF16, F32, F32)],
        (a, wg, wu) + (dy,) * last, scratch=[pltpu.VMEM((t, n), BF16)] * last, **carry,
    )


def down_kernel(act, wd, h, **carry):
    t, ff = act.shape
    d = wd.shape[1]
    m, n = 512, 256

    def body(ins, outs, own, mark):
        act, wd, h = ins
        new, a, at = outs
        for j in range(d // n):
            cols = pl.ds(j * n, n)
            new[:, cols] = h[:, cols] + dot(act[...], wd[:, cols], (1, 0)).astype(BF16)
            mark(j)
        a[...] = scaled(new[...])
        at[...] = a[...].T

    row = lambda cols: pl.BlockSpec((m, cols), lambda i: (i, 0))
    return hosted(
        "down", body, t // m, d // n, [row(ff), whole((ff, d)), row(d)], [row(d)] * 2 + [pl.BlockSpec((d, m), lambda i: (0, i))],
        [jax.ShapeDtypeStruct((t, d), BF16)] * 2 + [jax.ShapeDtypeStruct((d, t), BF16)], (act, wd, h), **carry,
    )


def back_kernel(dh, wd, s, v, act=None, at=None, **carry):
    t, d = dh.shape
    ff = s.shape[1]
    n, part = 256, 512
    down = act is not None

    def body(ins, outs, own, mark):
        dh, wd, s, v, other = ins
        by_g, by_u = outs[:2]
        for j in range(t // part):
            rows = pl.ds(j * part, part)
            by_act = dot(dh[rows, :], wd[...], (1, 1)).astype(BF16).astype(F32)
            by_g[rows, :] = (by_act * v[rows, :]).astype(BF16)
            by_u[rows, :] = (by_act * s[rows, :]).astype(BF16)
        mark(0)
        if down:
            outs[2][...] = dot(other[...], dh[...], (0, 0)).astype(BF16)
        else:
            outs[2][...] = dot(other[...], by_g[...], (1, 0)).astype(BF16)
            outs[3][...] = dot(other[...], by_u[...], (1, 0)).astype(BF16)
        mark(1)

    col = lambda rows: pl.BlockSpec((rows, n), lambda i: (0, i))
    row = pl.BlockSpec((n, d), lambda i: (i, 0))
    shape = lambda *s: jax.ShapeDtypeStruct(s, BF16)
    return hosted(
        "back", body, ff // n, 2, [whole((t, d)), row, col(t), col(t), col(t) if down else whole((d, t))],
        [col(t)] * 2 + ([row] if down else [col(d)] * 2),
        [shape(t, ff)] * 2 + ([shape(ff, d)] if down else [shape(d, ff)] * 2),
        (dh, wd, s, v, act if down else at), **carry,
    )


def outer_kernel(at, by_g, by_u, **carry):
    d, t = at.shape
    ff = by_g.shape[1]
    n = 256

    def body(ins, outs, own, mark):
        at, by_g, by_u = ins
        for by, out in ((by_g, outs[0]), (by_u, outs[1])):
            out[...] = dot(at[...], by[...], (1, 0)).astype(BF16)
        mark(0)

    col = lambda rows: pl.BlockSpec((rows, n), lambda i: (0, i))
    return hosted(
        "outer", body, ff // n, 1, [whole((d, t)), col(t), col(t)], [col(d)] * 2, [jax.ShapeDtypeStruct((d, ff), BF16)] * 2,
        (at, by_g, by_u), **carry,
    )


def through_kernel(by_g, by_u, wg, wu, h, dh, **carry):
    t, ff = by_g.shape
    d = wg.shape[0]
    m, n = 256, 256

    def body(ins, outs, own, mark):
        by_g, by_u, wg, wu, h, dh = ins
        (new,) = outs
        (by_a,) = own
        for j in range(d // n):
            cols = pl.ds(j * n, n)
            one = dot(by_g[...], wg[cols, :], (1, 1)).astype(BF16)
            two = dot(by_u[...], wu[cols, :], (1, 1)).astype(BF16)
            by_a[:, cols] = (one + two).astype(F32)
            mark(j)
        wide, by = h[...].astype(F32), by_a[...]
        scale = lax.rsqrt(jnp.mean(wide * wide, -1, keepdims=True) + 1e-6)
        inner = jnp.mean(wide * by, -1, keepdims=True)
        new[...] = dh[...] + (by * scale - wide * (scale * scale * scale * inner)).astype(BF16)

    row = lambda cols: pl.BlockSpec((m, cols), lambda i: (i, 0))
    return hosted(
        "through", body, t // m, d // n, [row(ff), row(ff), whole((d, ff)), whole((d, ff)), row(d), row(d)], [row(d)],
        [jax.ShapeDtypeStruct((t, d), BF16)], (by_g, by_u, wg, wu, h, dh), scratch=[pltpu.VMEM((m, d), F32)], **carry,
    )


def alone(name, **carry):
    return hosted(name, None, 1, 1, [], [], [], (), **carry)[1]


def adamw(w, m, v, g):
    m = 0.9 * m + 0.1 * g
    v = 0.95 * v + 0.05 * g * g
    step = m * lax.rsqrt(v + 1e-8) + 0.1 * w
    return (w - 0.02 * step).astype(BF16), m, v


def clipped(gradients, sum_of_squares, count):
    factor = jnp.minimum(1.0, 0.5 * lax.rsqrt(sum_of_squares / count + 1e-30))
    return [g * factor for g in gradients]


def solution(mesh):
    def step(x, dy, *arrays):
        weights, m, v = (arrays[i : i + 3] for i in (0, 3, 6))
        w_gate, w_up, w_down = weights
        wide, deep = w_gate.shape[1:], w_down.shape[1:]
        x, dy = x[0], dy[0]

        tile = 128
        pair = [(m, at * tile, side * tile, (13 - side) * tile) for m in range(2) for at, side in ((0, 4), (13, 5))]
        single = [(0, at * tile, side * tile, (4 - side) * tile) for at, side in ((0, 1), (4, 2))]
        two = lambda layer, number: dict(carried=Gather([wide, wide], pair, layer), carried_args=(w_gate, w_up), number=number)
        one = lambda layer, number: dict(carried=Gather([deep], single, layer), carried_args=(w_down,), number=number)
        total = lambda shape, by, number: dict(carried=Scatter([shape], 2), carried_args=(by,), number=number)

        (a0, at0), (wg0, wu0) = norm_kernel(x, **two(0, 1))
        (act0, s0, v0), (wd0,) = up_kernel(a0, wg0, wu0, **one(0, 2))
        (h1, a1, at1), (wg1, wu1) = down_kernel(act0, wd0, x, **two(1, 3))
        (s1, v1, by_d1), (wd1,) = up_kernel(a1, wg1, wu1, dy, **one(1, 4))

        (by_g, by_u, by_g1, by_u1), (sd1, q1) = back_kernel(dy, wd1, s1, v1, at=at1, **total(deep, by_d1, 5))
        (dh,), (sg1, q2) = through_kernel(by_g, by_u, wg1, wu1, h1, dy, **total(wide, by_g1, 6))
        (by_g, by_u, by_d0), (su1, q3) = back_kernel(dh, wd0, s0, v0, act=act0, **total(wide, by_u1, 7))
        (by_g0, by_u0), (sd0, q4) = outer_kernel(at0, by_g, by_u, **total(deep, by_d0, 8))
        last = Scatter([wide, wide], 2, everyone=True)
        sg0, su0, squares = alone("scatter", carried=last, carried_args=(by_g0, by_u0, q1 + q2 + q3 + q4), number=9)

        mine = ((sg0, sg1), (su0, su1), (sd0, sd1))
        gradients = [jnp.stack(pair).astype(F32) for pair in mine]
        gradients = clipped(gradients, squares[0, 0], lax.psum(1, "dp") * sum(g.size for g in gradients))
        new = [adamw(w.astype(F32), m, v, g) for w, m, v, g in zip(weights, m, v, gradients, strict=True)]
        return tuple(one[which] for which in range(3) for one in new)

    states, cut = P(("rep", "dp"), None, None), P(None, "dp", None)
    return jax.shard_map(
        step,
        mesh=mesh,
        in_specs=(states, states) + (cut,) * 9,
        out_specs=(P("rep", "dp", None),) * 9,
        check_vma=False,
    )
```

```python
import functools

import jax
import jax.numpy as jnp
from jax import lax
from jax.experimental import pallas as pl
from jax.experimental.pallas import tpu as pltpu
from jax.sharding import PartitionSpec as P

BF16, F32 = jnp.bfloat16, jnp.float32
MIB = 1 << 20
CHIPS = 8
ANY = pl.BlockSpec(memory_space=pl.ANY)


def order(q):
    return q + lax.div(q, 4) * (11 - 2 * q)


class Here:
    def __init__(self):
        me = lax.axis_index("dp")
        self.me, self.c = me, lax.rem(me, 2)
        self.p = order(lax.div(me, 2))
        self.sibling = {"dp": 2 * lax.div(me, 2) + 1 - self.c}
        self.hops = (4 - self.c, 3 + self.c)
        self.rep = lax.axis_index("rep")
        self.twin = {"rep": 1 - self.rep}
        self.next = tuple({"dp": 2 * self.chip(o) + self.c} for o in (1, CHIPS - 1))

    def chip(self, offset):
        return order(lax.rem(self.p + offset, CHIPS))


def remote(src, dst, send, recv, to):
    return pltpu.make_async_remote_copy(src, dst, send, recv, device_id=to, device_id_type=pl.DeviceIdType.MESH)


def greet(*others):
    barrier = pltpu.get_barrier_semaphore()
    for to in others:
        pl.semaphore_signal(barrier, inc=1, device_id=to, device_id_type=pl.DeviceIdType.MESH)
    pl.semaphore_wait(barrier, len(others))


class Gather:
    def __init__(self, shapes, units, number):
        self.shapes, self.number = shapes, number
        self.units = [(m, at, side, ring) for m, at, side, ring in units]
        n = len(self.units)
        self.rounds = 6 * n
        dma = pltpu.SemaphoreType.DMA
        self.scratch = [dma((n, 2, 4)), dma((n, 2, 4)), *[dma((n, CHIPS))] * 6, dma((len(shapes),))]
        self.scratch += [pltpu.VMEM(shape, BF16) for shape in shapes]
        self.out_shapes = [jax.ShapeDtypeStruct((2 * CHIPS * r, c), BF16) for r, c in shapes]

    def bind(self, ins, outs, scratch):
        self.ins, self.outs = [ref.at[self.number] for ref in ins], outs
        self.send, self.recv, self.dsend, self.drecv, self.xsend, self.xrecv, self.tsend, self.trecv, self.local = scratch[:9]
        self.held = scratch[9:]

    def columns(self, here, u, kind):
        m, at, side, ring = self.units[u]
        if kind == "all":
            return pl.ds(at, side + ring)
        if kind == "ring":
            return pl.ds(pl.multiple_of(at + here.rep * side, 128), ring)
        rep = here.rep if kind == "gives" else 1 - here.rep
        return pl.ds(pl.multiple_of(at + rep * ring, 128), side)

    def block(self, here, u, offset, kind):
        m = self.units[u][0]
        rows = self.shapes[m][0]
        start = pl.multiple_of((2 * here.chip(offset) + here.c) * rows, 16)
        return self.outs[m].at[pl.ds(start, rows), self.columns(here, u, kind)]

    def own(self, here, u, kind):
        return self.ins[self.units[u][0]].at[:, self.columns(here, u, kind)]

    def start(self, here):
        greet(here.sibling, here.twin, *here.next)
        for m in range(len(self.shapes)):
            pltpu.make_async_copy(self.ins[m], self.held[m], self.local.at[m]).start()

    def unit(self, here, u, h):
        @pl.when(h == 0)
        def _():
            mine, dst = self.own(here, u, "ring"), self.block(here, u, 0, "ring")
            for d in range(2):
                remote(mine, dst, self.send.at[u, d, 0], self.recv.at[u, d, 0], here.next[d]).start()
            mine, dst = self.own(here, u, "all"), self.block(here, u, 0, "all")
            remote(mine, dst, self.dsend.at[u, 0], self.drecv.at[u, 0], here.sibling).start()

        for d in range(2):
            offset = lax.rem(CHIPS - h, CHIPS) if d == 0 else lax.rem(h, CHIPS)
            blk = self.block(here, u, offset, "ring")

            @pl.when((h >= 1) & (h <= here.hops[d]))
            def _():
                remote(blk, blk, self.send.at[u, d, h - 1], self.recv.at[u, d, h - 1], here.next[d]).wait_recv()

            @pl.when((h >= 1) & (h < here.hops[d]))
            def _():
                remote(blk, blk, self.send.at[u, d, h], self.recv.at[u, d, h], here.next[d]).start()

            @pl.when((h >= 1) & (h <= here.hops[d]))
            def _():
                part = self.block(here, u, offset, "gives")
                remote(part, part, self.xsend.at[u, offset], self.xrecv.at[u, offset], here.twin).start()
                remote(blk, blk, self.dsend.at[u, offset], self.drecv.at[u, offset], here.sibling).start()

        for d in range(2):
            before = lax.rem(CHIPS + 1 - h, CHIPS) if d == 0 else lax.rem(CHIPS + h - 1, CHIPS)

            @pl.when((h >= 2) & (h - 1 <= here.hops[d]))
            def _():
                part = self.block(here, u, before, "gets")
                remote(part, part, self.xsend.at[u, before], self.xrecv.at[u, before], here.twin).wait_recv()
                remote(part, part, self.tsend.at[u, before], self.trecv.at[u, before], here.sibling).start()

    def round(self, here, r):
        n = len(self.units)
        for u in range(n):
            pl.when(lax.rem(r, n) == u)(functools.partial(self.unit, here, u, lax.div(r, n)))

    def rows(self, here, m):
        rows = self.shapes[m][0]
        return self.outs[m].at[pl.ds(pl.multiple_of(here.me * rows, 16), rows), :]

    def finish(self, here):
        for m in range(len(self.shapes)):
            pltpu.make_async_copy(self.ins[m], self.held[m], self.local.at[m]).wait()
            pltpu.make_async_copy(self.held[m], self.rows(here, m), self.local.at[m]).start()
        for u in range(len(self.units)):
            blk = self.block(here, u, 0, "all")
            remote(blk, blk, self.dsend.at[u, 0], self.drecv.at[u, 0], here.sibling).wait()

            @pl.loop(1, CHIPS)
            def _(o):
                blk = self.block(here, u, o, "ring")
                remote(blk, blk, self.dsend.at[u, o], self.drecv.at[u, o], here.sibling).wait()
                blk = self.block(here, u, o, "gives")
                remote(blk, blk, self.xsend.at[u, o], self.xrecv.at[u, o], here.twin).wait_send()
                blk = self.block(here, u, o, "gets")
                remote(blk, blk, self.tsend.at[u, o], self.trecv.at[u, o], here.sibling).wait()

            for d in range(2):

                @pl.loop(0, here.hops[d])
                def _(h):
                    blk = self.block(here, u, 0, "ring")
                    remote(blk, blk, self.send.at[u, d, h], self.recv.at[u, d, h], here.next[d]).wait_send()

        for m in range(len(self.shapes)):
            pltpu.make_async_copy(self.held[m], self.rows(here, m), self.local.at[m]).wait()


class Scatter:
    def __init__(self, shapes, cuts, everyone=False):
        self.shapes, self.cuts, self.everyone = shapes, cuts, everyone
        self.units = [(m, i, shape[0], shape[1] // cuts) for m, shape in enumerate(shapes) for i in range(cuts)]
        n = len(self.units)
        self.rounds = 5 * n
        dma = pltpu.SemaphoreType.DMA
        self.scratch = [dma((n, 2, 4)), dma((n, 2, 4)), dma((n, CHIPS)), dma((n, CHIPS)), dma((n, CHIPS))]
        for _, _, rows, cols in self.units:
            self.scratch += [pltpu.VMEM((CHIPS, rows, cols), BF16)] * 2 + [pltpu.VMEM((2, 4, rows, cols), BF16)]
        self.scratch += [pltpu.VMEM(shape, BF16) for shape in shapes] + [dma((len(shapes) + 1,))]
        self.scratch += [pltpu.VMEM((8, 128), F32), pltpu.VMEM((2 * CHIPS, 8, 128), F32), dma((2 * CHIPS,)), dma((2 * CHIPS,))]
        self.out_shapes = [*(jax.ShapeDtypeStruct(shape, BF16) for shape in shapes), jax.ShapeDtypeStruct((8, 128), F32)]

    def bind(self, ins, outs, scratch):
        self.ins, self.outs = ins, outs
        self.send, self.recv, self.dsend, self.drecv, self.local = scratch[:5]
        n = len(self.units)
        self.mine, self.theirs, self.came = (scratch[5 + j : 5 + 3 * n : 3] for j in range(3))
        self.total = scratch[5 + 3 * n : -5]
        self.put, self.squares, self.slots, self.psend, self.precv = scratch[-5:]

    def term(self, here, u, offset, core):
        m, i, rows, cols = self.units[u]
        start = pl.multiple_of((2 * here.chip(offset) + core) * rows, 16)
        return self.ins[m].at[pl.ds(start, rows), pl.ds(i * cols, cols)]

    def fetch(self, here, u, o):
        return pltpu.make_async_copy(self.term(here, u, o, here.c), self.mine[u].at[o], self.local.at[u, o])

    def give(self, here, u, o):
        term = self.term(here, u, o, 1 - here.c)
        return remote(term, self.theirs[u].at[o], self.dsend.at[u, o], self.drecv.at[u, o], here.sibling)

    def peer(self, here, j):
        return {"dp": lax.rem(here.me + j, 2 * CHIPS)}

    def start(self, here):
        if self.everyone:
            greet(*(self.peer(here, j) for j in range(1, 2 * CHIPS)))
            pltpu.make_async_copy(self.ins[-1], self.squares, self.put.at[len(self.shapes)]).start()
        else:
            greet(here.sibling, *here.next)
        for k in range(2):
            for u in range(len(self.units)):
                self.ahead(here, u, k)

    def ahead(self, here, u, k):
        for d in range(2):
            far = here.hops[d] - k
            o = lax.rem(far + CHIPS if d == 0 else CHIPS - far, CHIPS)

            @pl.when(k < here.hops[d])
            def _():
                self.give(here, u, o).start()
                self.fetch(here, u, o).start()

    def unit(self, here, u, k):
        m, i, rows, cols = self.units[u]
        mine, theirs, came = self.mine[u], self.theirs[u], self.came[u]
        self.ahead(here, u, k + 2)

        @pl.when(k == 1)
        def _():
            self.give(here, u, 0).start()
            self.fetch(here, u, 0).start()

        for d in range(2):
            far = here.hops[d] - k
            o = lax.rem(far + CHIPS if d == 0 else CHIPS - far, CHIPS)

            @pl.when(k < here.hops[d])
            def _():
                self.fetch(here, u, o).wait()
                self.give(here, u, o).wait_recv()

            @pl.when((k < here.hops[d]) & (k == 0))
            def _():
                mine[o] = (mine[o].astype(F32) + theirs[o].astype(F32)).astype(BF16)

            @pl.when((k < here.hops[d]) & (k > 0))
            def _():
                remote(mine.at[o], came.at[d, k - 1], self.send.at[u, d, k - 1], self.recv.at[u, d, k - 1], here.next[d]).wait_recv()
                mine[o] = (mine[o].astype(F32) + theirs[o].astype(F32) + came[d, k - 1].astype(F32)).astype(BF16)

            @pl.when(k < here.hops[d])
            def _():
                remote(mine.at[o], came.at[d, k], self.send.at[u, d, k], self.recv.at[u, d, k], here.next[d]).start()

        @pl.when(k == 4)
        def _():
            self.fetch(here, u, 0).wait()
            self.give(here, u, 0).wait_recv()
            total = mine[0].astype(F32) + theirs[0].astype(F32)
            for d in range(2):
                last = here.hops[d] - 1
                remote(mine.at[0], came.at[d, last], self.send.at[u, d, last], self.recv.at[u, d, last], here.next[d]).wait_recv()
                total += came[d, last].astype(F32)
            self.total[m][:, pl.ds(i * cols, cols)] = total.astype(BF16)

    def round(self, here, r):
        n = len(self.units)
        for u in range(n):
            pl.when(lax.rem(r, n) == u)(functools.partial(self.unit, here, u, lax.div(r, n)))

    def finish(self, here):
        n = len(self.shapes)
        for m in range(n):
            pltpu.make_async_copy(self.total[m], self.outs[m], self.put.at[m]).start()
        squares = 0.0
        for m in range(n):
            wide = self.total[m][...].astype(F32)
            squares += jnp.sum(wide * wide)
        squares = jnp.full((8, 128), squares, F32)
        if self.everyone:
            pltpu.make_async_copy(self.ins[-1], self.squares, self.put.at[n]).wait()
            self.slots[here.me] = self.squares[...] + squares

            @pl.loop(1, 2 * CHIPS)
            def _(j):
                slot = self.slots.at[here.me]
                remote(slot, slot, self.psend.at[j], self.precv.at[here.me], self.peer(here, j)).start()

            @pl.loop(1, 2 * CHIPS)
            def _(j):
                other = lax.rem(here.me + j, 2 * CHIPS)
                slot = self.slots.at[other]
                remote(slot, slot, self.psend.at[j], self.precv.at[other], self.peer(here, j)).wait()

            squares = jnp.sum(self.slots[...], axis=0)
        self.squares[...] = squares
        pltpu.make_async_copy(self.squares, self.outs[n], self.put.at[n]).start()
        for u in range(len(self.units)):

            @pl.loop(0, CHIPS)
            def _(o):
                self.give(here, u, o).wait_send()

            for d in range(2):

                @pl.loop(0, here.hops[d])
                def _(k):
                    remote(
                        self.mine[u].at[0], self.came[u].at[d, k], self.send.at[u, d, k], self.recv.at[u, d, k], here.next[d]
                    ).wait_send()

        for m in range(n):
            pltpu.make_async_copy(self.total[m], self.outs[m], self.put.at[m]).wait()
        pltpu.make_async_copy(self.squares, self.outs[n], self.put.at[n]).wait()


def hosted(name, body, steps, marks, in_specs, out_specs, out_shape, args, carried=None, carried_args=(), number=None, scratch=(), limit=60):
    n_in, n_out, n_scratch = len(in_specs), len(out_specs), len(scratch)
    n_cin = len(carried_args)
    c_out = carried.out_shapes if carried else []

    def kernel(*refs):
        ins, refs = refs[:n_in], refs[n_in:]
        cin, refs = refs[:n_cin], refs[n_cin:]
        outs, refs = refs[:n_out], refs[n_out:]
        couts, refs = refs[: len(c_out)], refs[len(c_out) :]
        own, refs = refs[:n_scratch], refs[n_scratch:]
        step = pl.program_id(0)
        if carried is None:
            body(ins, outs, own, lambda j: None)
            return
        here = Here()
        carried.bind(cin, couts, refs)
        pl.when(step == 0)(functools.partial(carried.start, here))
        total = steps * marks

        def mark(j):
            at = step * marks + j

            @pl.loop(lax.div(at * carried.rounds, total), lax.div((at + 1) * carried.rounds, total))
            def _(r):
                carried.round(here, r)

        if body is None:
            mark(0)
        else:
            body(ins, outs, own, mark)
        pl.when(step == steps - 1)(functools.partial(carried.finish, here))

    params = dict(vmem_limit_bytes=limit * MIB, dimension_semantics=("arbitrary",))
    if carried is not None:
        params |= dict(collective_id=number, has_side_effects=True)
    out = pl.pallas_call(
        kernel,
        grid=(steps,),
        in_specs=[*in_specs, *[ANY] * n_cin],
        out_specs=[*out_specs, *[ANY] * len(c_out)],
        out_shape=[*out_shape, *c_out],
        scratch_shapes=[*scratch, *(carried.scratch if carried else [])],
        compiler_params=pltpu.CompilerParams(**params),
        name=name,
    )(*args, *carried_args)
    return out[:n_out], out[n_out:]


def whole(shape):
    return pl.BlockSpec(shape, lambda i: (0, 0), pipeline_mode=pl.Buffered(1))


def dot(a, b, over):
    return lax.dot_general(a, b, ((over[:1], over[1:]), ((), ())), preferred_element_type=F32)


def scaled(h):
    wide = h.astype(F32)
    return (wide * lax.rsqrt(jnp.mean(wide * wide, -1, keepdims=True) + 1e-6)).astype(BF16)


def norm_kernel(x, **carry):
    t, d = x.shape
    m = 512

    def body(ins, outs, own, mark):
        a = scaled(ins[0][...])
        outs[0][...] = a
        outs[1][...] = a.T
        mark(0)

    row = pl.BlockSpec((m, d), lambda i: (i, 0))
    return hosted(
        "norm", body, t // m, 1, [row], [row, pl.BlockSpec((d, m), lambda i: (0, i))],
        [jax.ShapeDtypeStruct((t, d), BF16), jax.ShapeDtypeStruct((d, t), BF16)], (x,), **carry,
    )


def up_kernel(a, wg, wu, dy=None, **carry):
    t, d = a.shape
    ff = wg.shape[1]
    n, part = 256, 512
    last = dy is not None

    def body(ins, outs, own, mark):
        a, wg, wu = ins[:3]
        act, s, v = (*own, *outs[:2]) if last else outs
        for j in range(t // part):
            rows = pl.ds(j * part, part)
            g = dot(a[rows, :], wg[...], (1, 0))
            u = dot(a[rows, :], wu[...], (1, 0))
            sig = jax.nn.sigmoid(g)
            sl = g * sig
            act[rows, :] = (sl * u).astype(BF16)
            s[rows, :] = sl
            v[rows, :] = u * (sig * (1.0 + g * (1.0 - sig)))
        if last:
            outs[2][...] = dot(act[...], ins[3][...], (0, 0)).astype(BF16)
        mark(0)

    col = lambda rows: pl.BlockSpec((rows, n), lambda i: (0, i))
    row = pl.BlockSpec((n, d), lambda i: (i, 0))
    return hosted(
        "up", body, ff // n, 1, [whole((t, d)), col(d), col(d)] + [whole((t, d))] * last,
        [col(t)] * 2 + [row] if last else [col(t)] * 3,
        [jax.ShapeDtypeStruct((t, ff), F32)] * 2 + [jax.ShapeDtypeStruct((ff, d), BF16)]
        if last else [jax.ShapeDtypeStruct((t, ff), x) for x in (BF16, F32, F32)],
        (a, wg, wu) + (dy,) * last, scratch=[pltpu.VMEM((t, n), BF16)] * last, **carry,
    )


def down_kernel(act, wd, h, **carry):
    t, ff = act.shape
    d = wd.shape[1]
    m, n = 512, 512

    def body(ins, outs, own, mark):
        act, wd, h = ins
        new, a, at = outs

        @pl.loop(0, d // n)
        def _(j):
            cols = pl.ds(pl.multiple_of(j * n, n), n)
            new[:, cols] = h[:, cols] + dot(act[...], wd[:, cols], (1, 0)).astype(BF16)
            mark(j)
        a[...] = scaled(new[...])
        at[...] = a[...].T

    row = lambda cols: pl.BlockSpec((m, cols), lambda i: (i, 0))
    return hosted(
        "down", body, t // m, d // n, [row(ff), whole((ff, d)), row(d)], [row(d)] * 2 + [pl.BlockSpec((d, m), lambda i: (0, i))],
        [jax.ShapeDtypeStruct((t, d), BF16)] * 2 + [jax.ShapeDtypeStruct((d, t), BF16)], (act, wd, h), **carry,
    )


def back_kernel(dh, wd, s, v, act=None, at=None, **carry):
    t, d = dh.shape
    ff = s.shape[1]
    n, part = 256, 512
    down = act is not None

    def body(ins, outs, own, mark):
        dh, wd, s, v, other = ins
        by_g, by_u = outs[:2]
        for j in range(t // part):
            rows = pl.ds(j * part, part)
            by_act = dot(dh[rows, :], wd[...], (1, 1)).astype(BF16).astype(F32)
            by_g[rows, :] = (by_act * v[rows, :]).astype(BF16)
            by_u[rows, :] = (by_act * s[rows, :]).astype(BF16)
        mark(0)
        if down:
            outs[2][...] = dot(other[...], dh[...], (0, 0)).astype(BF16)
        else:
            outs[2][...] = dot(other[...], by_g[...], (1, 0)).astype(BF16)
            outs[3][...] = dot(other[...], by_u[...], (1, 0)).astype(BF16)
        mark(1)

    col = lambda rows: pl.BlockSpec((rows, n), lambda i: (0, i))
    row = pl.BlockSpec((n, d), lambda i: (i, 0))
    shape = lambda *s: jax.ShapeDtypeStruct(s, BF16)
    return hosted(
        "back", body, ff // n, 2, [whole((t, d)), row, col(t), col(t), col(t) if down else whole((d, t))],
        [col(t)] * 2 + ([row] if down else [col(d)] * 2),
        [shape(t, ff)] * 2 + ([shape(ff, d)] if down else [shape(d, ff)] * 2),
        (dh, wd, s, v, act if down else at), **carry,
    )


def outer_kernel(at, by_g, by_u, **carry):
    d, t = at.shape
    ff = by_g.shape[1]
    n = 256

    def body(ins, outs, own, mark):
        at, by_g, by_u = ins
        for by, out in ((by_g, outs[0]), (by_u, outs[1])):
            out[...] = dot(at[...], by[...], (1, 0)).astype(BF16)
        mark(0)

    col = lambda rows: pl.BlockSpec((rows, n), lambda i: (0, i))
    return hosted(
        "outer", body, ff // n, 1, [whole((d, t)), col(t), col(t)], [col(d)] * 2, [jax.ShapeDtypeStruct((d, ff), BF16)] * 2,
        (at, by_g, by_u), **carry,
    )


def through_kernel(by_g, by_u, wg, wu, h, dh, **carry):
    t, ff = by_g.shape
    d = wg.shape[0]
    m, n = 512, 256

    def body(ins, outs, own, mark):
        by_g, by_u, wg, wu, h, dh = ins
        (new,) = outs
        (by_a,) = own

        @pl.loop(0, d // n)
        def _(j):
            cols = pl.ds(pl.multiple_of(j * n, n), n)
            one = dot(by_g[...], wg[cols, :], (1, 1)).astype(BF16)
            two = dot(by_u[...], wu[cols, :], (1, 1)).astype(BF16)
            by_a[:, cols] = (one + two).astype(F32)
            mark(j)
        wide, by = h[...].astype(F32), by_a[...]
        scale = lax.rsqrt(jnp.mean(wide * wide, -1, keepdims=True) + 1e-6)
        inner = jnp.mean(wide * by, -1, keepdims=True)
        new[...] = dh[...] + (by * scale - wide * (scale * scale * scale * inner)).astype(BF16)

    row = lambda cols: pl.BlockSpec((m, cols), lambda i: (i, 0))
    return hosted(
        "through", body, t // m, d // n, [row(ff), row(ff), whole((d, ff)), whole((d, ff)), row(d), row(d)], [row(d)],
        [jax.ShapeDtypeStruct((t, d), BF16)], (by_g, by_u, wg, wu, h, dh), scratch=[pltpu.VMEM((m, d), F32)], **carry,
    )


def alone(name, **carry):
    return hosted(name, None, 1, 1, [], [], [], (), **carry)[1]


def adamw(w, m, v, g):
    m = 0.9 * m + 0.1 * g
    v = 0.95 * v + 0.05 * g * g
    step = m * lax.rsqrt(v + 1e-8) + 0.1 * w
    return (w - 0.02 * step).astype(BF16), m, v


def clipped(gradients, sum_of_squares, count):
    factor = jnp.minimum(1.0, 0.5 * lax.rsqrt(sum_of_squares / count + 1e-30))
    return [g * factor for g in gradients]


def solution(mesh):
    def step(x, dy, *arrays):
        weights, m, v = (arrays[i : i + 3] for i in (0, 3, 6))
        w_gate, w_up, w_down = weights
        wide, deep = w_gate.shape[1:], w_down.shape[1:]
        x, dy = x[0], dy[0]

        tile = 128
        pair = [(m, at * tile, side * tile, (13 - side) * tile) for m in range(2) for at, side in ((0, 4), (13, 4))]
        single = [(0, at * tile, side * tile, (4 - side) * tile) for at, side in ((0, 1), (4, 1))]
        two = lambda layer, number: dict(carried=Gather([wide, wide], pair, layer), carried_args=(w_gate, w_up), number=number)
        one = lambda layer, number: dict(carried=Gather([deep], single, layer), carried_args=(w_down,), number=number)
        total = lambda shape, by, number: dict(carried=Scatter([shape], 2), carried_args=(by,), number=number)

        (a0, at0), (wg0, wu0) = norm_kernel(x, **two(0, 1))
        (act0, s0, v0), (wd0,) = up_kernel(a0, wg0, wu0, **one(0, 2))
        (h1, a1, at1), (wg1, wu1) = down_kernel(act0, wd0, x, **two(1, 3))
        (s1, v1, by_d1), (wd1,) = up_kernel(a1, wg1, wu1, dy, **one(1, 4))

        (by_g, by_u, by_g1, by_u1), (sd1, q1) = back_kernel(dy, wd1, s1, v1, at=at1, **total(deep, by_d1, 5))
        (dh,), (sg1, q2) = through_kernel(by_g, by_u, wg1, wu1, h1, dy, **total(wide, by_g1, 6))
        (by_g, by_u, by_d0), (su1, q3) = back_kernel(dh, wd0, s0, v0, act=act0, **total(wide, by_u1, 7))
        (by_g0, by_u0), (sd0, q4) = outer_kernel(at0, by_g, by_u, **total(deep, by_d0, 8))
        last = Scatter([wide, wide], 2, everyone=True)
        sg0, su0, squares = alone("scatter", carried=last, carried_args=(by_g0, by_u0, q1 + q2 + q3 + q4), number=9)

        mine = ((sg0, sg1), (su0, su1), (sd0, sd1))
        gradients = [jnp.stack(pair).astype(F32) for pair in mine]
        gradients = clipped(gradients, squares[0, 0], lax.psum(1, "dp") * sum(g.size for g in gradients))
        new = [adamw(w.astype(F32), m, v, g) for w, m, v, g in zip(weights, m, v, gradients, strict=True)]
        return tuple(one[which] for which in range(3) for one in new)

    states, cut = P(("rep", "dp"), None, None), P(None, "dp", None)
    return jax.shard_map(
        step,
        mesh=mesh,
        in_specs=(states, states) + (cut,) * 9,
        out_specs=(P("rep", "dp", None),) * 9,
        check_vma=False,
    )
```
